32 devices in a mesh: grp: 4 (over y, x), dev: 8 (over z, core).
Axes of the slice: x: 2, y: 2, z: 4, core: 2. Of those that a mesh axis runs over, the one named last changes fastest.
Arguments:
- positions: float32 [3, 32768], P(None, ('grp', 'dev')), may hold values from -6 to 6
- velocities: float32 [3, 32768], P(None, ('grp', 'dev')), may hold values from -6 to 6
- masses: float32 [32768], P(('grp', 'dev')), may hold values from 0.2 to 5
- active_index: int32 [1024], replicated, may hold values from 0 to 32767, as said below
Outputs:
- force: float32 [3, 1024], P(None, ('grp', 'dev'))
- jerk: float32 [3, 1024], P(None, ('grp', 'dev'))
The draws below stay inside these ranges and needn't reach their ends.
Inputs may be any that keep to these rules, and one draw needn't show every extreme that they name: `active_index`: strictly increasing, distinct indices of stars; at most 64 of them fall in any aligned block of 1024 consecutive stars, and some block holds exactly 64.
All inputs are finite; a program needn't handle non-finite values.
Results may differ from the reference program's by a relative error of at most 0.0003.
Values sent between devices are 32-bit elements; how exact they have to be, the bound alone decides.
A program may use at most 64 MiB of HBM per device.

```python
import math
import jax
import jax.numpy as jnp
from jax import lax

STARS_DEV = 1024
ACTIVE = 1024
STARS = 32768


def draw_active_index(key, part):
    ndev = STARS // STARS_DEV
    mean = ACTIVE // ndev
    pattern = jnp.tile(jnp.array([2, 1, 1, 0], jnp.int32) * mean, ndev // 4)
    order_dev = jax.random.permutation(jax.random.fold_in(key, 11), ndev)
    counts = pattern[order_dev]
    top = max(2, 2 ** 30 // STARS_DEV)
    scores = jax.random.randint(jax.random.fold_in(key, 13), (ndev, STARS_DEV), 0, top, dtype=jnp.int32)
    scores = scores * STARS_DEV + jnp.arange(STARS_DEV, dtype=jnp.int32)[None, :]
    order = jnp.argsort(scores, axis=1)
    ranks = jnp.argsort(order, axis=1)
    chosen = (ranks < counts[:, None]).reshape(-1)
    picked = jnp.nonzero(chosen, size=ACTIVE, fill_value=0)[0]
    return picked.astype(jnp.int32)


def shard_levels(key, extent, cuts, smallest, top_value):
    gain = 1.0
    for axis_at, shards_of in cuts:
        draws = jax.random.uniform(jax.random.fold_in(jax.random.fold_in(key, 6), axis_at), (shards_of,), jnp.float32, smallest / len(cuts), top_value / len(cuts))
        gain = gain * jnp.repeat(jnp.exp(draws), extent[axis_at] // shards_of).reshape((-1,) + (1,) * (len(extent) - 1 - axis_at))
    return gain


def normal_values(rng, shape, spread, reach, cuts=(), kind=jnp.bfloat16):
    level = shard_levels(rng, shape, cuts, -0.22, 0.18) if cuts else 1.0
    values = jax.random.normal(rng, shape, jnp.float32) * spread * level
    return jnp.minimum(jnp.maximum(values, -reach), reach).astype(kind)


def setup_inputs(seed: int = 0) -> dict:
    seeds = jax.random.split(jax.random.key(seed), 5)
    positions = normal_values(seeds[0], (3, STARS), 1.0, 6.0, ((1, 32),), jnp.float32)
    velocities = normal_values(seeds[1], (3, STARS), 1.0, 6.0, ((1, 32),), jnp.float32)
    masses = jnp.clip(jnp.exp(math.log(5.0) - 3.218876 * jax.random.uniform(seeds[2], (STARS,), jnp.float32) ** shard_levels(seeds[2], (STARS,), ((0, 32),), -0.2, 0.2)), 0.2, 5.0)
    active_index = draw_active_index(jax.random.fold_in(seeds[4], 71), 0)
    return dict(positions=positions, velocities=velocities, masses=masses, active_index=active_index)


SOFT = 0.0025

def pair_terms(act_pos, act_vel, pos, vel, mass):
    dx = pos[:, None, :] - act_pos[:, :, None]
    dv = vel[:, None, :] - act_vel[:, :, None]
    r2 = lax.optimization_barrier(jnp.sum(dx * dx, axis=0)) + SOFT
    inv = 1.0 / jnp.sqrt(r2)
    weight = mass[None, :] * inv * inv * inv
    rv = lax.optimization_barrier(jnp.sum(dx * dv, axis=0))
    acc = lax.optimization_barrier(jnp.sum(weight[None] * dx, axis=-1))
    jer = lax.optimization_barrier(jnp.sum(weight[None] * dv - (3.0 * rv * weight / r2)[None] * dx, axis=-1))
    return (acc, jer)

def reference(positions, velocities, masses, active_index):
    block = min(256, ACTIVE)
    star_block = min(16384, STARS)
    act_pos = jnp.take(positions, active_index, axis=1)
    act_vel = jnp.take(velocities, active_index, axis=1)
    nblk = ACTIVE // block
    nstar = STARS // star_block
    apos = act_pos.reshape(3, nblk, block).transpose(1, 0, 2)
    avel = act_vel.reshape(3, nblk, block).transpose(1, 0, 2)
    spos = positions.reshape(3, nstar, star_block).transpose(1, 0, 2)
    svel = velocities.reshape(3, nstar, star_block).transpose(1, 0, 2)
    smass = masses.reshape(nstar, star_block)

    def one_block(item):
        bpos, bvel = item

        def step(carry, piece):
            acc, jer = pair_terms(bpos, bvel, piece[0], piece[1], piece[2])
            return ((carry[0] + acc, carry[1] + jer), None)
        zeros = jnp.zeros((3, block), jnp.float32)
        (acc, jer), _ = lax.scan(step, (zeros, zeros), (spos, svel, smass))
        return (acc, jer)
    acc, jer = lax.map(one_block, (apos, avel))
    scale = 1.0 / STARS
    force = acc.transpose(1, 0, 2).reshape(3, ACTIVE) * scale
    jerk = jer.transpose(1, 0, 2).reshape(3, ACTIVE) * scale
    return (force, jerk)
```

```python
import functools

import jax
import jax.numpy as jnp
from jax import lax
from jax.experimental import pallas as pl
from jax.experimental.pallas import tpu as pltpu
from jax.sharding import PartitionSpec as P

SOFT = 0.0025
SUB, LANE = 8, 128
HALF = LANE // 2
UNROLL = 8


def pair_terms(act_pos, act_vel, pos, vel, mass):
    dx = pos[:, None, :] - act_pos[:, :, None]
    dv = vel[:, None, :] - act_vel[:, :, None]
    r2 = jnp.sum(dx * dx, axis=0) + SOFT
    inv = 1.0 / jnp.sqrt(r2)
    weight = mass[None, :] * inv * inv * inv
    rv = jnp.sum(dx * dv, axis=0)
    acc = jnp.sum(weight[None] * dx, axis=-1)
    jer = jnp.sum(weight[None] * dv - (3.0 * rv * weight / r2)[None] * dx, axis=-1)
    return (acc, jer)


def per_device(positions, velocities, masses, active_index):
    local_count = positions.shape[1]
    groups = lax.axis_size("grp")
    members = lax.axis_size("dev")
    active = active_index.shape[0]
    owner = lax.axis_index("grp") * members + lax.axis_index("dev")
    offset = owner * local_count
    local = active_index - offset
    owned = (local >= 0) & (local < local_count)
    clipped = jnp.clip(local, 0, local_count - 1)
    state = jnp.concatenate(
        [jnp.take(positions, clipped, axis=1), jnp.take(velocities, clipped, axis=1)], axis=0
    )
    state = jnp.where(owned[None, :], state, 0.0)
    state = lax.psum(state, ("grp", "dev"))
    block = min(256, active)
    nblk = active // block
    blocks = state.reshape(6, nblk, block).transpose(1, 0, 2)

    def one_block(item):
        return pair_terms(item[0:3], item[3:6], positions, velocities, masses)

    acc, jer = lax.map(one_block, blocks)
    scale = 1.0 / (local_count * groups * members)
    both = jnp.concatenate(
        [acc.transpose(1, 0, 2).reshape(3, active), jer.transpose(1, 0, 2).reshape(3, active)], axis=0
    )
    both = lax.psum_scatter(both * scale, ("grp", "dev"), scatter_dimension=1, tiled=True)
    return (both[0:3], both[3:6])


def kernel(groups, members, idx_ref, pos_ref, vel_ref, pos_s, vel_s, mass_s, force_ref, jerk_ref,
           mine, got, part, parts, send_a, recv_a, send_b, recv_b):
    ndev = groups * members
    count = pos_ref.shape[1]
    per = force_ref.shape[1]
    ngrp = LANE // per
    me = lax.axis_index("grp") * members + lax.axis_index("dev")

    def place(k):
        other = lax.rem(me + k, ndev)
        return other, (lax.div(other, members), lax.rem(other, members))

    barrier = pltpu.get_barrier_semaphore()

    def greet(k, c):
        pl.semaphore_signal(barrier, inc=1, device_id=place(k)[1], device_id_type=pl.DeviceIdType.MESH)
        return c

    lax.fori_loop(1, ndev, greet, 0)

    idx = idx_ref[...]
    local = idx - me * count
    owned = (local >= 0) & (local < count)
    slot = jnp.sum(jnp.where(owned, local + 1, 0), axis=0, keepdims=True)
    slot = slot + pltpu.roll(slot, HALF, 1)
    pick = (lax.broadcasted_iota(jnp.int32, (count, LANE), 0) + 1 == slot).astype(jnp.float32)
    up = jnp.dot(pos_ref[...], pick, precision=lax.Precision.HIGHEST, preferred_element_type=jnp.float32)
    uv = jnp.dot(vel_ref[...], pick, precision=lax.Precision.HIGHEST, preferred_element_type=jnp.float32)
    lane3 = lax.broadcasted_iota(jnp.int32, (3, LANE), 1)
    own = jnp.where(lane3 < HALF, up, uv)
    mine[...] = own
    got[me] = own

    pl.semaphore_wait(barrier, ndev - 1)

    def gather_copy(k, sender):
        other, where = place(k)
        return pltpu.make_async_remote_copy(
            src_ref=mine, dst_ref=got.at[sender], send_sem=send_a.at[other], recv_sem=recv_a.at[sender],
            device_id=where, device_id_type=pl.DeviceIdType.MESH)

    def start_a(k, c):
        gather_copy(k, me).start()
        return c

    def wait_a(k, c):
        gather_copy(k, place(k)[0]).wait_recv()
        return c

    def sent_a(k, c):
        gather_copy(k, me).wait_send()
        return c

    lax.fori_loop(1, ndev, start_a, 0)
    lax.fori_loop(1, ndev, wait_a, 0)

    same = [jnp.zeros((SUB, LANE), jnp.float32)] * 3
    swap = [jnp.zeros((SUB, LANE), jnp.float32)] * 3
    for d in range(ndev):
        rows = got[d]
        turned = pltpu.roll(rows, HALF, 1)
        from_d = idx >= d * count
        for i in range(3):
            same[i] = jnp.where(from_d, jnp.broadcast_to(rows[i:i + 1], (SUB, LANE)), same[i])
            swap[i] = jnp.where(from_d, jnp.broadcast_to(turned[i:i + 1], (SUB, LANE)), swap[i])
    lane = lax.broadcasted_iota(jnp.int32, (SUB, LANE), 1)
    ap = [jnp.where(lane < HALF, same[i], swap[i]) for i in range(3)]
    av = [jnp.where(lane < HALF, swap[i], same[i]) for i in range(3)]

    def step(b, sums):
        sums = list(sums)
        for u in range(UNROLL):
            j = b * UNROLL + u
            dx = [pos_s[i, j] - ap[i] for i in range(3)]
            dv = [vel_s[i, j] - av[i] for i in range(3)]
            r2 = dx[0] * dx[0] + dx[1] * dx[1] + (dx[2] * dx[2] + SOFT)
            inv = lax.rsqrt(r2)
            inv2 = inv * inv
            weight = (mass_s[j] * inv) * inv2
            rv = dx[0] * dv[0] + dx[1] * dv[1] + dx[2] * dv[2]
            bend = (rv * inv2) * weight
            for i in range(3):
                sums[i] = sums[i] + weight * dx[i]
                sums[3 + i] = sums[3 + i] + weight * dv[i]
                sums[6 + i] = sums[6 + i] + bend * dx[i]
        return tuple(sums)

    zero = jnp.zeros((SUB, LANE), jnp.float32)
    sums = lax.fori_loop(0, count // UNROLL, step, (zero,) * 9)
    scale = 1.0 / (count * ndev)
    outs = [sums[i] * scale for i in range(3)]
    outs += [(sums[3 + i] - 3.0 * sums[6 + i]) * scale for i in range(3)]

    kind = lax.div(lane, per)
    nrow = part.shape[2]
    for g in range(ngrp):
        for r in range(nrow):
            packed = zero
            for f in range(min(ngrp, 6 - ngrp * r)):
                value = outs[ngrp * r + f]
                turn = per * ((f - g) % ngrp)
                if turn:
                    value = pltpu.roll(value, turn, 1)
                packed = jnp.where(kind == f, value, packed)
            part[:, g, r, :] = packed

    def scatter_copy(k, sender):
        other, where = place(k)
        return pltpu.make_async_remote_copy(
            src_ref=part.at[lax.div(other, ngrp), lax.rem(other, ngrp)], dst_ref=parts.at[sender],
            send_sem=send_b.at[other], recv_sem=recv_b.at[sender],
            device_id=where, device_id_type=pl.DeviceIdType.MESH)

    def start_b(k, c):
        scatter_copy(k, me).start()
        return c

    def wait_b(k, c):
        scatter_copy(k, place(k)[0]).wait_recv()
        return c

    def sent_b(k, c):
        scatter_copy(k, me).wait_send()
        return c

    lax.fori_loop(1, ndev, start_b, 0)
    parts[me] = part[lax.div(me, ngrp), lax.rem(me, ngrp)]
    lax.fori_loop(1, ndev, sent_a, 0)
    lax.fori_loop(1, ndev, wait_b, 0)
    total = jnp.sum(parts[...], axis=0)
    for f in range(6):
        r, c = f // ngrp, (f % ngrp) * per
        out_ref = force_ref if f < 3 else jerk_ref
        out_ref[f % 3:f % 3 + 1, :] = total[r:r + 1, c:c + per]
    lax.fori_loop(1, ndev, sent_b, 0)


def fused(groups, members, positions, velocities, masses, active_index):
    ndev = groups * members
    per = active_index.shape[0] // ndev
    ngrp = LANE // per
    nrow = -(-6 // ngrp)
    vmem = pl.BlockSpec(memory_space=pltpu.VMEM)
    smem = pl.BlockSpec(memory_space=pltpu.SMEM)
    out = jax.ShapeDtypeStruct((3, per), jnp.float32)
    sems = pltpu.SemaphoreType.DMA((ndev,))
    return pl.pallas_call(
        functools.partial(kernel, groups, members),
        out_shape=(out, out),
        in_specs=[vmem, vmem, vmem, smem, smem, smem],
        out_specs=(vmem, vmem),
        scratch_shapes=[
            pltpu.VMEM((3, LANE), jnp.float32),
            pltpu.VMEM((ndev, 3, LANE), jnp.float32),
            pltpu.VMEM((ndev // ngrp, ngrp, nrow, LANE), jnp.float32),
            pltpu.VMEM((ndev, nrow, LANE), jnp.float32),
            sems, sems, sems, sems,
        ],
        compiler_params=pltpu.CompilerParams(collective_id=0, has_side_effects=True),
        name="hermite",
    )(active_index.reshape(SUB, LANE), positions, velocities, positions, velocities, masses)


def solution(mesh):
    groups, members = mesh.shape["grp"], mesh.shape["dev"]
    ndev = groups * members

    def body(positions, velocities, masses, active_index):
        active, count = active_index.shape[0], positions.shape[1]
        per = active // ndev
        fits = active == SUB * LANE and LANE % per == 0 and ndev == SUB * (LANE // per)
        if fits and 2 * per == HALF and count % UNROLL == 0:
            return fused(groups, members, positions, velocities, masses, active_index)
        return per_device(positions, velocities, masses, active_index)

    return jax.shard_map(
        body,
        mesh=mesh,
        in_specs=(P(None, ("grp", "dev")), P(None, ("grp", "dev")), P(("grp", "dev")), P()),
        out_specs=(P(None, ("grp", "dev")), P(None, ("grp", "dev"))),
        check_vma=False,
    )
```

```python
import functools

import jax
import jax.numpy as jnp
from jax import lax
from jax.experimental import pallas as pl
from jax.experimental.pallas import tpu as pltpu
from jax.sharding import PartitionSpec as P

SOFT = 0.0025
SUB, LANE = 8, 128
HALF = LANE // 2
UNROLL = 8


def pair_terms(act_pos, act_vel, pos, vel, mass):
    dx = pos[:, None, :] - act_pos[:, :, None]
    dv = vel[:, None, :] - act_vel[:, :, None]
    r2 = jnp.sum(dx * dx, axis=0) + SOFT
    inv = 1.0 / jnp.sqrt(r2)
    weight = mass[None, :] * inv * inv * inv
    rv = jnp.sum(dx * dv, axis=0)
    acc = jnp.sum(weight[None] * dx, axis=-1)
    jer = jnp.sum(weight[None] * dv - (3.0 * rv * weight / r2)[None] * dx, axis=-1)
    return (acc, jer)


def per_device(positions, velocities, masses, active_index):
    local_count = positions.shape[1]
    groups = lax.axis_size("grp")
    members = lax.axis_size("dev")
    active = active_index.shape[0]
    owner = lax.axis_index("grp") * members + lax.axis_index("dev")
    offset = owner * local_count
    local = active_index - offset
    owned = (local >= 0) & (local < local_count)
    clipped = jnp.clip(local, 0, local_count - 1)
    state = jnp.concatenate(
        [jnp.take(positions, clipped, axis=1), jnp.take(velocities, clipped, axis=1)], axis=0
    )
    state = jnp.where(owned[None, :], state, 0.0)
    state = lax.psum(state, ("grp", "dev"))
    block = min(256, active)
    nblk = active // block
    blocks = state.reshape(6, nblk, block).transpose(1, 0, 2)

    def one_block(item):
        return pair_terms(item[0:3], item[3:6], positions, velocities, masses)

    acc, jer = lax.map(one_block, blocks)
    scale = 1.0 / (local_count * groups * members)
    both = jnp.concatenate(
        [acc.transpose(1, 0, 2).reshape(3, active), jer.transpose(1, 0, 2).reshape(3, active)], axis=0
    )
    both = lax.psum_scatter(both * scale, ("grp", "dev"), scatter_dimension=1, tiled=True)
    return (both[0:3], both[3:6])


def kernel(groups, members, idx_h, pos_h, vel_h, mass_h, both_ref,
           idx_ref, stars, mass_ref, wide, got, part, parts,
           load_sem, send_g, recv_g, send_d, recv_d, send_b, recv_b):
    ndev = groups * members
    count = pos_h.shape[1]
    chunks = count // LANE
    per = both_ref.shape[2]
    ngrp = LANE // per
    my_g, my_d = lax.axis_index("grp"), lax.axis_index("dev")
    me = my_g * members + my_d

    barrier = pltpu.get_barrier_semaphore()
    for k in range(1, groups):
        pl.semaphore_signal(barrier, inc=1, device_id=(lax.rem(my_g + k, groups), my_d),
                            device_id_type=pl.DeviceIdType.MESH)
    for k in range(1, members):
        pl.semaphore_signal(barrier, inc=1, device_id=(my_g, lax.rem(my_d + k, members)),
                            device_id_type=pl.DeviceIdType.MESH)

    loads = [
        pltpu.make_async_copy(idx_h, idx_ref, load_sem.at[0]),
        pltpu.make_async_copy(pos_h, stars.at[0], load_sem.at[1]),
        pltpu.make_async_copy(vel_h, stars.at[1], load_sem.at[2]),
        pltpu.make_async_copy(mass_h, mass_ref, load_sem.at[3]),
    ]
    for copy in loads:
        copy.start()
    for copy in loads:
        copy.wait()

    idx = idx_ref[...]
    local = idx - me * count
    owned = (local >= 0) & (local < count)
    slot = jnp.sum(jnp.where(owned, local + 1, 0), axis=0, keepdims=True)
    slot = slot + pltpu.roll(slot, HALF, 1)
    pick = (lax.broadcasted_iota(jnp.int32, (count, LANE), 0) + 1 == slot).astype(jnp.float32)
    state = jnp.concatenate([stars[0], stars[1]], axis=0)
    picked = jnp.dot(state, pick, precision=lax.Precision.HIGHEST, preferred_element_type=jnp.float32)
    lane3 = lax.broadcasted_iota(jnp.int32, (3, LANE), 1)
    got[my_d, my_g] = jnp.where(lane3 < HALF, picked[0:3], picked[3:6])

    pl.semaphore_wait(barrier, groups + members - 2)

    def group_copy(k, sender):
        g = lax.rem(my_g + k, groups)
        return pltpu.make_async_remote_copy(
            src_ref=got.at[my_d, my_g], dst_ref=got.at[my_d, sender],
            send_sem=send_g.at[g], recv_sem=recv_g.at[sender],
            device_id=(g, my_d), device_id_type=pl.DeviceIdType.MESH)

    def member_copy(k, sender):
        d = lax.rem(my_d + k, members)
        return pltpu.make_async_remote_copy(
            src_ref=got.at[my_d], dst_ref=got.at[sender],
            send_sem=send_d.at[d], recv_sem=recv_d.at[sender],
            device_id=(my_g, d), device_id_type=pl.DeviceIdType.MESH)

    for k in range(1, groups):
        group_copy(k, my_g).start()

    def spread(c, carry):
        at = pl.ds(pl.multiple_of(c * LANE, LANE), LANE)
        rows = jnp.concatenate(
            [stars[0, :, at], stars[1, :, at], mass_ref[pl.ds(c, 1), :], mass_ref[pl.ds(c, 1), :]], axis=0)
        cols = jnp.transpose(rows)
        for f in range(7):
            wide[f, at, :] = jnp.broadcast_to(cols[:, f:f + 1], (LANE, LANE))
        return carry

    first = chunks // 4
    lax.fori_loop(0, first, spread, 0)
    for k in range(1, groups):
        group_copy(k, lax.rem(my_g + k, groups)).wait_recv()
    for k in range(1, members):
        member_copy(k, my_d).start()
    lax.fori_loop(first, chunks, spread, 0)
    for k in range(1, members):
        member_copy(k, lax.rem(my_d + k, members)).wait_recv()

    same = [jnp.zeros((SUB, LANE), jnp.float32)] * 3
    swap = [jnp.zeros((SUB, LANE), jnp.float32)] * 3
    for d in range(ndev):
        rows = got[d % members, d // members]
        turned = pltpu.roll(rows, HALF, 1)
        from_d = idx >= d * count
        for i in range(3):
            same[i] = jnp.where(from_d, jnp.broadcast_to(rows[i:i + 1], (SUB, LANE)), same[i])
            swap[i] = jnp.where(from_d, jnp.broadcast_to(turned[i:i + 1], (SUB, LANE)), swap[i])
    lane = lax.broadcasted_iota(jnp.int32, (SUB, LANE), 1)
    ap = [jnp.where(lane < HALF, same[i], swap[i]) for i in range(3)]
    av = [jnp.where(lane < HALF, swap[i], same[i]) for i in range(3)]

    def step(b, sums):
        sums = list(sums)
        base = pl.multiple_of(b * UNROLL, UNROLL)
        for u in range(UNROLL):
            star = [jnp.broadcast_to(wide[f, pl.ds(base + u, 1), :], (SUB, LANE)) for f in range(7)]
            dx = [star[i] - ap[i] for i in range(3)]
            dv = [star[3 + i] - av[i] for i in range(3)]
            r2 = dx[0] * dx[0] + dx[1] * dx[1] + (dx[2] * dx[2] + SOFT)
            inv = lax.rsqrt(r2)
            inv2 = inv * inv
            weight = (star[6] * inv) * inv2
            rv = dx[0] * dv[0] + dx[1] * dv[1] + dx[2] * dv[2]
            bend = (rv * inv2) * weight
            for i in range(3):
                sums[i] = sums[i] + weight * dx[i]
                sums[3 + i] = sums[3 + i] + weight * dv[i]
                sums[6 + i] = sums[6 + i] + bend * dx[i]
        return tuple(sums)

    zero = jnp.zeros((SUB, LANE), jnp.float32)
    sums = lax.fori_loop(0, count // UNROLL, step, (zero,) * 9)
    scale = 1.0 / (count * ndev)
    outs = [sums[i] * scale for i in range(3)]
    outs += [(sums[3 + i] - 3.0 * sums[6 + i]) * scale for i in range(3)]

    kind = lax.div(lane, per)
    nrow = part.shape[2]
    for g in range(ngrp):
        for r in range(nrow):
            packed = zero
            for f in range(min(ngrp, 6 - ngrp * r)):
                value = outs[ngrp * r + f]
                turn = per * ((f - g) % ngrp)
                if turn:
                    value = pltpu.roll(value, turn, 1)
                packed = jnp.where(kind == f, value, packed)
            part[:, g, r, :] = packed

    def scatter_copy(k, sender):
        other = lax.rem(me + k, ndev)
        return pltpu.make_async_remote_copy(
            src_ref=part.at[lax.div(other, ngrp), lax.rem(other, ngrp)], dst_ref=parts.at[sender],
            send_sem=send_b.at[other], recv_sem=recv_b.at[sender],
            device_id=(lax.div(other, members), lax.rem(other, members)),
            device_id_type=pl.DeviceIdType.MESH)

    def start_b(k, c):
        scatter_copy(k, me).start()
        return c

    def wait_b(k, c):
        scatter_copy(k, lax.rem(me + k, ndev)).wait_recv()
        return c

    def sent_b(k, c):
        scatter_copy(k, me).wait_send()
        return c

    lax.fori_loop(1, ndev, start_b, 0)
    parts[me] = part[lax.div(me, ngrp), lax.rem(me, ngrp)]
    for k in range(1, groups):
        group_copy(k, my_g).wait_send()
    for k in range(1, members):
        member_copy(k, my_d).wait_send()
    lax.fori_loop(1, ndev, sent_b, 0)
    lax.fori_loop(1, ndev, wait_b, 0)
    total = jnp.sum(parts[...], axis=0)
    for f in range(6):
        r, c = f // ngrp, (f % ngrp) * per
        both_ref[f // 3, f % 3:f % 3 + 1, :] = total[r:r + 1, c:c + per]


def fused(groups, members, positions, velocities, masses, active_index):
    ndev = groups * members
    count = positions.shape[1]
    per = active_index.shape[0] // ndev
    ngrp = LANE // per
    nrow = -(-6 // ngrp)
    sems = pltpu.SemaphoreType.DMA
    both = pl.pallas_call(
        functools.partial(kernel, groups, members),
        out_shape=jax.ShapeDtypeStruct((2, 3, per), jnp.float32),
        in_specs=[pl.BlockSpec(memory_space=pl.ANY)] * 4,
        out_specs=pl.BlockSpec(memory_space=pltpu.VMEM),
        scratch_shapes=[
            pltpu.VMEM((SUB, LANE), jnp.int32),
            pltpu.VMEM((2, 3, count), jnp.float32),
            pltpu.VMEM((count // LANE, LANE), jnp.float32),
            pltpu.VMEM((7, count, LANE), jnp.float32),
            pltpu.VMEM((members, groups, 3, LANE), jnp.float32),
            pltpu.VMEM((ndev // ngrp, ngrp, nrow, LANE), jnp.float32),
            pltpu.VMEM((ndev, nrow, LANE), jnp.float32),
            sems((4,)), sems((groups,)), sems((groups,)), sems((members,)), sems((members,)),
            sems((ndev,)), sems((ndev,)),
        ],
        compiler_params=pltpu.CompilerParams(collective_id=0, has_side_effects=True),
        name="hermite",
    )(active_index.reshape(SUB, LANE), positions, velocities, masses.reshape(count // LANE, LANE))
    return both[0], both[1]


def solution(mesh):
    groups, members = mesh.shape["grp"], mesh.shape["dev"]
    ndev = groups * members

    def body(positions, velocities, masses, active_index):
        active, count = active_index.shape[0], positions.shape[1]
        per = active // ndev
        fits = active == SUB * LANE and LANE % per == 0 and ndev == SUB * (LANE // per)
        if fits and 2 * per == HALF and count % (SUB * LANE) == 0:
            return fused(groups, members, positions, velocities, masses, active_index)
        return per_device(positions, velocities, masses, active_index)

    return jax.shard_map(
        body,
        mesh=mesh,
        in_specs=(P(None, ("grp", "dev")), P(None, ("grp", "dev")), P(("grp", "dev")), P()),
        out_specs=(P(None, ("grp", "dev")), P(None, ("grp", "dev"))),
        check_vma=False,
    )
```

```python
import functools

import jax
import jax.numpy as jnp
from jax import lax
from jax.experimental import pallas as pl
from jax.experimental.pallas import tpu as pltpu
from jax.sharding import PartitionSpec as P

SOFT = 0.0025
SUB, LANE = 8, 128
HALF = LANE // 2
UNROLL = 16


def pair_terms(act_pos, act_vel, pos, vel, mass):
    dx = pos[:, None, :] - act_pos[:, :, None]
    dv = vel[:, None, :] - act_vel[:, :, None]
    r2 = jnp.sum(dx * dx, axis=0) + SOFT
    inv = 1.0 / jnp.sqrt(r2)
    weight = mass[None, :] * inv * inv * inv
    rv = jnp.sum(dx * dv, axis=0)
    acc = jnp.sum(weight[None] * dx, axis=-1)
    jer = jnp.sum(weight[None] * dv - (3.0 * rv * weight / r2)[None] * dx, axis=-1)
    return (acc, jer)


def per_device(positions, velocities, masses, active_index):
    local_count = positions.shape[1]
    groups = lax.axis_size("grp")
    members = lax.axis_size("dev")
    active = active_index.shape[0]
    owner = lax.axis_index("grp") * members + lax.axis_index("dev")
    offset = owner * local_count
    local = active_index - offset
    owned = (local >= 0) & (local < local_count)
    clipped = jnp.clip(local, 0, local_count - 1)
    state = jnp.concatenate(
        [jnp.take(positions, clipped, axis=1), jnp.take(velocities, clipped, axis=1)], axis=0
    )
    state = jnp.where(owned[None, :], state, 0.0)
    state = lax.psum(state, ("grp", "dev"))
    block = min(256, active)
    nblk = active // block
    blocks = state.reshape(6, nblk, block).transpose(1, 0, 2)

    def one_block(item):
        return pair_terms(item[0:3], item[3:6], positions, velocities, masses)

    acc, jer = lax.map(one_block, blocks)
    scale = 1.0 / (local_count * groups * members)
    both = jnp.concatenate(
        [acc.transpose(1, 0, 2).reshape(3, active), jer.transpose(1, 0, 2).reshape(3, active)], axis=0
    )
    both = lax.psum_scatter(both * scale, ("grp", "dev"), scatter_dimension=1, tiled=True)
    return (both[0:3], both[3:6])


def kernel(groups, members, idx_h, pos_h, vel_h, mass_h, both_ref,
           idx_ref, stars, mass_ref, wide, got, part, parts,
           load_sem, send_g, recv_g, send_d, recv_d, send_b, recv_b):
    ndev = groups * members
    count = pos_h.shape[1]
    chunks = count // LANE
    per = both_ref.shape[2]
    ngrp = LANE // per
    my_g, my_d = lax.axis_index("grp"), lax.axis_index("dev")
    me = my_g * members + my_d

    barrier = pltpu.get_barrier_semaphore()
    for k in range(1, groups):
        pl.semaphore_signal(barrier, inc=1, device_id=(lax.rem(my_g + k, groups), my_d),
                            device_id_type=pl.DeviceIdType.MESH)
    for k in range(1, members):
        pl.semaphore_signal(barrier, inc=1, device_id=(my_g, lax.rem(my_d + k, members)),
                            device_id_type=pl.DeviceIdType.MESH)

    loads = [
        pltpu.make_async_copy(idx_h, idx_ref, load_sem.at[0]),
        pltpu.make_async_copy(pos_h, stars.at[0], load_sem.at[1]),
        pltpu.make_async_copy(vel_h, stars.at[1], load_sem.at[2]),
        pltpu.make_async_copy(mass_h, mass_ref, load_sem.at[3]),
    ]
    for copy in loads:
        copy.start()
    loads[0].wait()

    idx = idx_ref[...]
    local = idx - me * count
    owned = (local >= 0) & (local < count)
    slot = jnp.sum(jnp.where(owned, local + 1, 0), axis=0, keepdims=True)
    slot = slot + pltpu.roll(slot, HALF, 1)
    pick = (lax.broadcasted_iota(jnp.int32, (count, LANE), 0) + 1 == slot).astype(jnp.float32)
    pick = pick.astype(jnp.bfloat16)
    for copy in loads[1:]:
        copy.wait()
    state = jnp.concatenate([stars[0], stars[1]], axis=0)
    high = state.astype(jnp.bfloat16).astype(jnp.float32)
    rest = state - high
    middle = rest.astype(jnp.bfloat16).astype(jnp.float32)
    fill = jnp.zeros((2, count), jnp.float32)
    pieces = jnp.concatenate([high, fill, middle, fill, rest - middle, fill], axis=0).astype(jnp.bfloat16)
    picked = jnp.dot(pieces, pick, preferred_element_type=jnp.float32)
    picked = (picked[0:8] + picked[8:16]) + picked[16:24]
    lane3 = lax.broadcasted_iota(jnp.int32, (3, LANE), 1)
    got[my_g, my_d] = jnp.where(lane3 < HALF, picked[0:3], picked[3:6])

    pl.semaphore_wait(barrier, groups + members - 2)

    def group_copy(k, sender):
        g = lax.rem(my_g + k, groups)
        return pltpu.make_async_remote_copy(
            src_ref=got.at[my_g], dst_ref=got.at[sender],
            send_sem=send_g.at[g], recv_sem=recv_g.at[sender],
            device_id=(g, my_d), device_id_type=pl.DeviceIdType.MESH)

    def member_copy(k, sender):
        d = lax.rem(my_d + k, members)
        return pltpu.make_async_remote_copy(
            src_ref=got.at[my_g, my_d], dst_ref=got.at[my_g, sender],
            send_sem=send_d.at[d], recv_sem=recv_d.at[sender],
            device_id=(my_g, d), device_id_type=pl.DeviceIdType.MESH)

    for k in range(1, members):
        member_copy(k, my_d).start()

    def spread(c, carry):
        at = pl.ds(pl.multiple_of(c * LANE, LANE), LANE)
        rows = jnp.concatenate(
            [stars[0, :, at], stars[1, :, at], mass_ref[pl.ds(c, 1), :], mass_ref[pl.ds(c, 1), :]], axis=0)
        cols = jnp.transpose(rows)
        for f in range(7):
            wide[f, at, :] = jnp.broadcast_to(cols[:, f:f + 1], (LANE, LANE))
        return carry

    first = chunks // 2
    lax.fori_loop(0, first, spread, 0)
    for k in range(1, members):
        member_copy(k, lax.rem(my_d + k, members)).wait_recv()
    for k in range(1, groups):
        group_copy(k, my_g).start()
    lax.fori_loop(first, chunks, spread, 0)
    for k in range(1, groups):
        group_copy(k, lax.rem(my_g + k, groups)).wait_recv()

    same = [jnp.zeros((SUB, LANE), jnp.float32)] * 3
    swap = [jnp.zeros((SUB, LANE), jnp.float32)] * 3
    for d in range(ndev):
        rows = got[d // members, d % members]
        turned = pltpu.roll(rows, HALF, 1)
        from_d = idx >= d * count
        for i in range(3):
            same[i] = jnp.where(from_d, jnp.broadcast_to(rows[i:i + 1], (SUB, LANE)), same[i])
            swap[i] = jnp.where(from_d, jnp.broadcast_to(turned[i:i + 1], (SUB, LANE)), swap[i])
    lane = lax.broadcasted_iota(jnp.int32, (SUB, LANE), 1)
    ap = [jnp.where(lane < HALF, same[i], swap[i]) for i in range(3)]
    av = [jnp.where(lane < HALF, swap[i], same[i]) for i in range(3)]

    def step(b, sums):
        sums = list(sums)
        base = pl.multiple_of(b * UNROLL, UNROLL)
        for u in range(UNROLL):
            star = [jnp.broadcast_to(wide[f, pl.ds(base + u, 1), :], (SUB, LANE)) for f in range(7)]
            dx = [star[i] - ap[i] for i in range(3)]
            dv = [star[3 + i] - av[i] for i in range(3)]
            r2 = dx[0] * dx[0] + dx[1] * dx[1] + (dx[2] * dx[2] + SOFT)
            inv = lax.rsqrt(r2)
            inv2 = inv * inv
            weight = (star[6] * inv) * inv2
            rv = dx[0] * dv[0] + dx[1] * dv[1] + dx[2] * dv[2]
            bend = (rv * inv2) * weight
            for i in range(3):
                sums[i] = sums[i] + weight * dx[i]
                sums[3 + i] = sums[3 + i] + weight * dv[i]
                sums[6 + i] = sums[6 + i] + bend * dx[i]
        return tuple(sums)

    zero = jnp.zeros((SUB, LANE), jnp.float32)
    sums = lax.fori_loop(0, count // UNROLL, step, (zero,) * 9)
    scale = 1.0 / (count * ndev)
    outs = [sums[i] * scale for i in range(3)]
    outs += [(sums[3 + i] - 3.0 * sums[6 + i]) * scale for i in range(3)]

    kind = lax.div(lane, per)
    nrow = part.shape[2]
    for g in range(ngrp):
        for r in range(nrow):
            packed = zero
            for f in range(min(ngrp, 6 - ngrp * r)):
                value = outs[ngrp * r + f]
                turn = per * ((f - g) % ngrp)
                if turn:
                    value = pltpu.roll(value, turn, 1)
                packed = jnp.where(kind == f, value, packed)
            part[:, g, r, :] = packed

    def scatter_copy(k, sender):
        other = lax.rem(me + k, ndev)
        return pltpu.make_async_remote_copy(
            src_ref=part.at[lax.div(other, ngrp), lax.rem(other, ngrp)], dst_ref=parts.at[sender],
            send_sem=send_b.at[other], recv_sem=recv_b.at[sender],
            device_id=(lax.div(other, members), lax.rem(other, members)),
            device_id_type=pl.DeviceIdType.MESH)

    def start_b(k, c):
        scatter_copy(k, me).start()
        return c

    def wait_b(k, c):
        scatter_copy(k, lax.rem(me + k, ndev)).wait_recv()
        return c

    def sent_b(k, c):
        scatter_copy(k, me).wait_send()
        return c

    lax.fori_loop(1, ndev, start_b, 0)
    parts[me] = part[lax.div(me, ngrp), lax.rem(me, ngrp)]
    for k in range(1, groups):
        group_copy(k, my_g).wait_send()
    for k in range(1, members):
        member_copy(k, my_d).wait_send()
    lax.fori_loop(1, ndev, sent_b, 0)
    lax.fori_loop(1, ndev, wait_b, 0)
    total = jnp.sum(parts[...], axis=0)
    for f in range(6):
        r, c = f // ngrp, (f % ngrp) * per
        both_ref[f // 3, f % 3:f % 3 + 1, :] = total[r:r + 1, c:c + per]


def fused(groups, members, positions, velocities, masses, active_index):
    ndev = groups * members
    count = positions.shape[1]
    per = active_index.shape[0] // ndev
    ngrp = LANE // per
    nrow = -(-6 // ngrp)
    sems = pltpu.SemaphoreType.DMA
    both = pl.pallas_call(
        functools.partial(kernel, groups, members),
        out_shape=jax.ShapeDtypeStruct((2, 3, per), jnp.float32),
        in_specs=[pl.BlockSpec(memory_space=pltpu.HBM)] * 4,
        out_specs=pl.BlockSpec(memory_space=pltpu.VMEM),
        scratch_shapes=[
            pltpu.VMEM((SUB, LANE), jnp.int32),
            pltpu.VMEM((2, 3, count), jnp.float32),
            pltpu.VMEM((count // LANE, LANE), jnp.float32),
            pltpu.VMEM((7, count, LANE), jnp.float32),
            pltpu.VMEM((groups, members, 3, LANE), jnp.float32),
            pltpu.VMEM((ndev // ngrp, ngrp, nrow, LANE), jnp.float32),
            pltpu.VMEM((ndev, nrow, LANE), jnp.float32),
            sems((4,)), sems((groups,)), sems((groups,)), sems((members,)), sems((members,)),
            sems((ndev,)), sems((ndev,)),
        ],
        compiler_params=pltpu.CompilerParams(collective_id=0, has_side_effects=True, vmem_limit_bytes=16 << 20),
        name="hermite",
    )(*[pltpu.with_memory_space_constraint(x, pltpu.HBM) for x in (
        active_index.reshape(SUB, LANE), positions, velocities, masses.reshape(count // LANE, LANE))])
    return both[0], both[1]


def solution(mesh):
    groups, members = mesh.shape["grp"], mesh.shape["dev"]
    ndev = groups * members

    def body(positions, velocities, masses, active_index):
        active, count = active_index.shape[0], positions.shape[1]
        per = active // ndev
        fits = active == SUB * LANE and LANE % per == 0 and ndev == SUB * (LANE // per)
        if fits and 2 * per == HALF and count % (SUB * LANE) == 0:
            return fused(groups, members, positions, velocities, masses, active_index)
        return per_device(positions, velocities, masses, active_index)

    return jax.shard_map(
        body,
        mesh=mesh,
        in_specs=(P(None, ("grp", "dev")), P(None, ("grp", "dev")), P(("grp", "dev")), P()),
        out_specs=(P(None, ("grp", "dev")), P(None, ("grp", "dev"))),
        check_vma=False,
    )
```

```python
import functools

import jax
import jax.numpy as jnp
from jax import lax
from jax.experimental import pallas as pl
from jax.experimental.pallas import tpu as pltpu
from jax.sharding import PartitionSpec as P

SOFT = 0.0025
SUB, LANE = 8, 128
HALF = LANE // 2
UNROLL = 16


def pair_terms(act_pos, act_vel, pos, vel, mass):
    dx = pos[:, None, :] - act_pos[:, :, None]
    dv = vel[:, None, :] - act_vel[:, :, None]
    r2 = jnp.sum(dx * dx, axis=0) + SOFT
    inv = 1.0 / jnp.sqrt(r2)
    weight = mass[None, :] * inv * inv * inv
    rv = jnp.sum(dx * dv, axis=0)
    acc = jnp.sum(weight[None] * dx, axis=-1)
    jer = jnp.sum(weight[None] * dv - (3.0 * rv * weight / r2)[None] * dx, axis=-1)
    return (acc, jer)


def per_device(positions, velocities, masses, active_index):
    local_count = positions.shape[1]
    groups = lax.axis_size("grp")
    members = lax.axis_size("dev")
    active = active_index.shape[0]
    owner = lax.axis_index("grp") * members + lax.axis_index("dev")
    offset = owner * local_count
    local = active_index - offset
    owned = (local >= 0) & (local < local_count)
    clipped = jnp.clip(local, 0, local_count - 1)
    state = jnp.concatenate(
        [jnp.take(positions, clipped, axis=1), jnp.take(velocities, clipped, axis=1)], axis=0
    )
    state = jnp.where(owned[None, :], state, 0.0)
    state = lax.psum(state, ("grp", "dev"))
    block = min(256, active)
    nblk = active // block
    blocks = state.reshape(6, nblk, block).transpose(1, 0, 2)

    def one_block(item):
        return pair_terms(item[0:3], item[3:6], positions, velocities, masses)

    acc, jer = lax.map(one_block, blocks)
    scale = 1.0 / (local_count * groups * members)
    both = jnp.concatenate(
        [acc.transpose(1, 0, 2).reshape(3, active), jer.transpose(1, 0, 2).reshape(3, active)], axis=0
    )
    both = lax.psum_scatter(both * scale, ("grp", "dev"), scatter_dimension=1, tiled=True)
    return (both[0:3], both[3:6])


def kernel(groups, members, idx_h, pos_h, vel_h, mass_h, both_ref,
           idx_ref, stars, mass_ref, wide, got, part, parts,
           load_sem, send_g, recv_g, send_d, recv_d, send_b, recv_b):
    ndev = groups * members
    count = pos_h.shape[1]
    chunks = count // LANE
    per = both_ref.shape[2]
    ngrp = LANE // per
    my_g, my_d = lax.axis_index("grp"), lax.axis_index("dev")
    me = my_g * members + my_d

    barrier = pltpu.get_barrier_semaphore()
    for k in range(1, groups):
        pl.semaphore_signal(barrier, inc=1, device_id=(lax.rem(my_g + k, groups), my_d),
                            device_id_type=pl.DeviceIdType.MESH)
    for k in range(1, members):
        pl.semaphore_signal(barrier, inc=1, device_id=(my_g, lax.rem(my_d + k, members)),
                            device_id_type=pl.DeviceIdType.MESH)

    loads = [
        pltpu.make_async_copy(idx_h, idx_ref, load_sem.at[0]),
        pltpu.make_async_copy(pos_h, stars.at[0], load_sem.at[1]),
        pltpu.make_async_copy(vel_h, stars.at[1], load_sem.at[2]),
        pltpu.make_async_copy(mass_h, mass_ref, load_sem.at[3]),
    ]
    for copy in loads:
        copy.start()
    loads[0].wait()

    idx = idx_ref[...]
    local = idx - me * count
    owned = (local >= 0) & (local < count)
    slot = jnp.sum(jnp.where(owned, local + 1, 0), axis=0, keepdims=True)
    slot = slot + pltpu.roll(slot, HALF, 1)
    pick = (lax.broadcasted_iota(jnp.int32, (count, LANE), 0) + 1 == slot).astype(jnp.float32)
    pick = pick.astype(jnp.bfloat16)
    for copy in loads[1:]:
        copy.wait()
    state = jnp.concatenate([stars[0], stars[1]], axis=0)
    high = state.astype(jnp.bfloat16).astype(jnp.float32)
    rest = state - high
    middle = rest.astype(jnp.bfloat16).astype(jnp.float32)
    fill = jnp.zeros((2, count), jnp.float32)
    pieces = jnp.concatenate([high, fill, middle, fill, rest - middle, fill], axis=0).astype(jnp.bfloat16)
    picked = jnp.dot(pieces, pick, preferred_element_type=jnp.float32)
    picked = (picked[0:8] + picked[8:16]) + picked[16:24]
    lane3 = lax.broadcasted_iota(jnp.int32, (3, LANE), 1)
    got[my_g, my_d] = jnp.where(lane3 < HALF, picked[0:3], picked[3:6])

    pl.semaphore_wait(barrier, groups + members - 2)

    def group_copy(k, sender):
        g = lax.rem(my_g + k, groups)
        return pltpu.make_async_remote_copy(
            src_ref=got.at[my_g], dst_ref=got.at[sender],
            send_sem=send_g.at[g], recv_sem=recv_g.at[sender],
            device_id=(g, my_d), device_id_type=pl.DeviceIdType.MESH)

    def member_copy(k, sender):
        d = lax.rem(my_d + k, members)
        return pltpu.make_async_remote_copy(
            src_ref=got.at[my_g, my_d], dst_ref=got.at[my_g, sender],
            send_sem=send_d.at[d], recv_sem=recv_d.at[sender],
            device_id=(my_g, d), device_id_type=pl.DeviceIdType.MESH)

    for k in range(1, members):
        member_copy(k, my_d).start()

    def spread(c, carry):
        at = pl.ds(pl.multiple_of(c * LANE, LANE), LANE)
        rows = jnp.concatenate(
            [stars[0, :, at], stars[1, :, at], mass_ref[pl.ds(c, 1), :], mass_ref[pl.ds(c, 1), :]], axis=0)
        cols = jnp.transpose(rows)
        for f in range(7):
            wide[f, at, :] = jnp.broadcast_to(cols[:, f:f + 1], (LANE, LANE))
        return carry

    first = chunks // 2
    lax.fori_loop(0, first, spread, 0)
    for k in range(1, members):
        member_copy(k, lax.rem(my_d + k, members)).wait_recv()
    for k in range(1, groups):
        group_copy(k, my_g).start()
    lax.fori_loop(first, chunks, spread, 0)
    for k in range(1, groups):
        group_copy(k, lax.rem(my_g + k, groups)).wait_recv()

    same = [jnp.zeros((SUB, LANE), jnp.float32)] * 3
    swap = [jnp.zeros((SUB, LANE), jnp.float32)] * 3
    for d in range(ndev):
        rows = got[d // members, d % members]
        turned = pltpu.roll(rows, HALF, 1)
        from_d = idx >= d * count
        for i in range(3):
            same[i] = jnp.where(from_d, jnp.broadcast_to(rows[i:i + 1], (SUB, LANE)), same[i])
            swap[i] = jnp.where(from_d, jnp.broadcast_to(turned[i:i + 1], (SUB, LANE)), swap[i])
    lane = lax.broadcasted_iota(jnp.int32, (SUB, LANE), 1)
    ap = [jnp.where(lane < HALF, same[i], swap[i]) for i in range(3)]
    av = [jnp.where(lane < HALF, swap[i], same[i]) for i in range(3)]

    def step(b, sums):
        sums = list(sums)
        base = pl.multiple_of(b * UNROLL, UNROLL)
        for u in range(UNROLL):
            star = [jnp.broadcast_to(wide[f, pl.ds(base + u, 1), :], (SUB, LANE)) for f in range(7)]
            dx = [star[i] - ap[i] for i in range(3)]
            dv = [star[3 + i] - av[i] for i in range(3)]
            r2 = dx[0] * dx[0] + dx[1] * dx[1] + (dx[2] * dx[2] + SOFT)
            inv = lax.rsqrt(r2)
            inv2 = inv * inv
            weight = (star[6] * inv) * inv2
            rv = dx[0] * dv[0] + dx[1] * dv[1] + dx[2] * dv[2]
            bend = (rv * inv2) * weight
            for i in range(3):
                sums[i] = sums[i] + weight * dx[i]
                sums[3 + i] = sums[3 + i] + weight * dv[i]
                sums[6 + i] = sums[6 + i] + bend * dx[i]
        return tuple(sums)

    zero = jnp.zeros((SUB, LANE), jnp.float32)
    sums = lax.fori_loop(0, count // UNROLL, step, (zero,) * 9)
    scale = 1.0 / (count * ndev)
    outs = [sums[i] * scale for i in range(3)]
    outs += [(sums[3 + i] - 3.0 * sums[6 + i]) * scale for i in range(3)]

    kind = lax.div(lane, per)
    nrow = part.shape[2]
    for g in range(ngrp):
        for r in range(nrow):
            packed = zero
            for f in range(min(ngrp, 6 - ngrp * r)):
                value = outs[ngrp * r + f]
                turn = per * ((f - g) % ngrp)
                if turn:
                    value = pltpu.roll(value, turn, 1)
                packed = jnp.where(kind == f, value, packed)
            part[:, g, r, :] = packed

    def scatter_copy(k, sender):
        other = lax.rem(me + k, ndev)
        return pltpu.make_async_remote_copy(
            src_ref=part.at[lax.div(other, ngrp), lax.rem(other, ngrp)], dst_ref=parts.at[sender],
            send_sem=send_b.at[other], recv_sem=recv_b.at[sender],
            device_id=(lax.div(other, members), lax.rem(other, members)),
            device_id_type=pl.DeviceIdType.MESH)

    def wait_b(k, c):
        scatter_copy(k, lax.rem(me + k, ndev)).wait_recv()
        return c

    def sent_b(k, c):
        scatter_copy(k, me).wait_send()
        return c

    places = [lax.rem(my_d + k, members) for k in range(members)]
    places = [(d, lax.div(d, ngrp), lax.rem(d, ngrp)) for d in places]
    for j in reversed(range(groups)):
        g = lax.rem(my_g + j, groups)
        for k in sorted(range(members), key=lambda k: abs(2 * k - members)):
            if j or k:
                d, block, turn = places[k]
                pltpu.make_async_remote_copy(
                    src_ref=part.at[g * (members // ngrp) + block, turn], dst_ref=parts.at[me],
                    send_sem=send_b.at[g * members + d], recv_sem=recv_b.at[me],
                    device_id=(g, d), device_id_type=pl.DeviceIdType.MESH).start()
    parts[me] = part[lax.div(me, ngrp), lax.rem(me, ngrp)]
    for k in range(1, groups):
        group_copy(k, my_g).wait_send()
    for k in range(1, members):
        member_copy(k, my_d).wait_send()
    lax.fori_loop(1, ndev, sent_b, 0)
    lax.fori_loop(1, ndev, wait_b, 0)
    total = jnp.sum(parts[...], axis=0)
    for f in range(6):
        r, c = f // ngrp, (f % ngrp) * per
        both_ref[f // 3, f % 3:f % 3 + 1, :] = total[r:r + 1, c:c + per]


def fused(groups, members, positions, velocities, masses, active_index):
    ndev = groups * members
    count = positions.shape[1]
    per = active_index.shape[0] // ndev
    ngrp = LANE // per
    nrow = -(-6 // ngrp)
    sems = pltpu.SemaphoreType.DMA
    both = pl.pallas_call(
        functools.partial(kernel, groups, members),
        out_shape=jax.ShapeDtypeStruct((2, 3, per), jnp.float32),
        in_specs=[pl.BlockSpec(memory_space=pltpu.HBM)] * 4,
        out_specs=pl.BlockSpec(memory_space=pltpu.VMEM),
        scratch_shapes=[
            pltpu.VMEM((SUB, LANE), jnp.int32),
            pltpu.VMEM((2, 3, count), jnp.float32),
            pltpu.VMEM((count // LANE, LANE), jnp.float32),
            pltpu.VMEM((7, count, LANE), jnp.float32),
            pltpu.VMEM((groups, members, 3, LANE), jnp.float32),
            pltpu.VMEM((ndev // ngrp, ngrp, nrow, LANE), jnp.float32),
            pltpu.VMEM((ndev, nrow, LANE), jnp.float32),
            sems((4,)), sems((groups,)), sems((groups,)), sems((members,)), sems((members,)),
            sems((ndev,)), sems((ndev,)),
        ],
        compiler_params=pltpu.CompilerParams(collective_id=0, has_side_effects=True, vmem_limit_bytes=16 << 20),
        name="hermite",
    )(*[pltpu.with_memory_space_constraint(x, pltpu.HBM) for x in (
        active_index.reshape(SUB, LANE), positions, velocities, masses.reshape(count // LANE, LANE))])
    return both[0], both[1]


def solution(mesh):
    groups, members = mesh.shape["grp"], mesh.shape["dev"]
    ndev = groups * members

    def body(positions, velocities, masses, active_index):
        active, count = active_index.shape[0], positions.shape[1]
        per = active // ndev
        fits = active == SUB * LANE and LANE % per == 0 and members % (LANE // per) == 0 and ndev == SUB * (LANE // per)
        if fits and 2 * per == HALF and count % (SUB * LANE) == 0:
            return fused(groups, members, positions, velocities, masses, active_index)
        return per_device(positions, velocities, masses, active_index)

    return jax.shard_map(
        body,
        mesh=mesh,
        in_specs=(P(None, ("grp", "dev")), P(None, ("grp", "dev")), P(("grp", "dev")), P()),
        out_specs=(P(None, ("grp", "dev")), P(None, ("grp", "dev"))),
        check_vma=False,
    )
```
